512 devices in a mesh: grp: 2 (over y), row: 32 (over z), col: 4 (over x), ch: 2 (over core).
Axes of the slice: x: 4, y: 2, z: 32, core: 2. Of those that a mesh axis runs over, the one named last changes fastest.
The devices are a block of a 4x8x32 slice.
Arguments:
- pair_act: bfloat16 [128, 1024, 512], P('ch', ('grp', 'row'), 'col'), parts along dimension 1, may hold values from -48 to 48
- in_gain: float32 [128], P('ch'), may hold values from 0.1 to 1.9
- left_proj: bfloat16 [128, 128], P(None, 'ch'), may hold values from -0.5 to 0.5
- left_gate: bfloat16 [128, 128], P(None, 'ch'), may hold values from -0.5 to 0.5
- right_proj: bfloat16 [128, 128], P(None, 'ch'), may hold values from -0.5 to 0.5
- right_gate: bfloat16 [128, 128], P(None, 'ch'), may hold values from -0.5 to 0.5
- out_gate: bfloat16 [128, 128], P(None, 'ch'), may hold values from -0.5 to 0.5
- out_gain: float32 [128], P('ch'), may hold values from 0.1 to 1.9
- out_proj: bfloat16 [128, 128], P(None, 'ch'), may hold values from -0.5 to 0.5
Outputs:
- update: bfloat16 [128, 1024, 512], P('ch', ('grp', 'row'), 'col'), parts along dimension 1
The draws below stay inside these ranges and needn't reach their ends.
There are 2 independent parts, one for each index of `grp`. The reference program is written for one: setup_inputs(seed, part) draws one part's arguments, and reference() takes and returns one part's arrays. A program takes and returns all parts, laid end to end along the dimension named above; an argument that names none is the same for every part. Nothing has to cross between parts.
All inputs are finite; a program needn't handle non-finite values.
Results may differ from the reference program's by a relative error of at most 0.0085.
Values may be sent and summed in bfloat16 or wider, within the bound.
A program may use at most 64 MiB of HBM per device.

```python
import jax
import jax.numpy as jnp
from jax import lax

C = 128
HID = 128
RES = 512


def draw_pair_act(key, part):
    keys = jax.random.split(jax.random.fold_in(key, 11), 4)
    base = jnp.clip(jax.random.normal(keys[0], (C, RES, RES), jnp.float32), -5.0, 5.0)
    channel_scale = jnp.exp(jax.random.uniform(keys[1], (C, 1, 1), jnp.float32, jnp.log(0.3), jnp.log(3.0)))
    site_scale = jnp.exp(jax.random.uniform(keys[2], (1, RES, RES), jnp.float32, jnp.log(0.3), jnp.log(3.0)))
    offset = 0.5 * jnp.clip(jax.random.normal(keys[3], (1, RES, RES), jnp.float32), -3.0, 3.0)
    return (base * channel_scale * site_scale + offset).astype(jnp.bfloat16)


def level_of(stream_key, extent, shards, low, largest):
    level = 1.0
    for position, parts in shards:
        heights = jax.random.uniform(jax.random.fold_in(jax.random.fold_in(stream_key, 6), position), (parts,), jnp.float32, low / len(shards), largest / len(shards))
        level = level * jnp.repeat(jnp.exp(heights), extent[position] // parts).reshape((-1,) + (1,) * (len(extent) - 1 - position))
    return level


def normal_values(own_key, extent, deviation, limit, shards=(), kind=jnp.bfloat16):
    entries = jax.random.normal(own_key, extent, jnp.float32) * deviation
    if len(shards) > 0:
        entries = level_of(own_key, extent, shards, -0.22, 0.18) * entries
    return jnp.clip(entries, min=-limit, max=limit).astype(kind)


def setup_inputs(seed: int = 0, part: int = 0) -> dict:
    key_list = jax.random.split(jax.random.key(seed), 10)
    part_splits = jax.random.split(jax.random.fold_in(key_list[9], part), 10)
    return {
        "pair_act": draw_pair_act(jax.random.fold_in(jax.random.fold_in(key_list[9], part), 71), part),
        "in_gain": jnp.clip(1.0 + 0.18 * jax.random.normal(key_list[1], (C,), jnp.float32), 0.1, 1.9),
        "left_proj": normal_values(key_list[2], (C, HID), C ** -0.5, 0.5, ((1, 2),)),
        "left_gate": normal_values(key_list[3], (C, HID), C ** -0.5, 0.5, ((1, 2),)),
        "right_proj": normal_values(key_list[4], (C, HID), C ** -0.5, 0.5, ((1, 2),)),
        "right_gate": normal_values(key_list[5], (C, HID), C ** -0.5, 0.5, ((1, 2),)),
        "out_gate": normal_values(key_list[6], (C, C), C ** -0.5, 0.5, ((1, 2),)),
        "out_gain": jnp.clip(1.0 + 0.18 * jax.random.normal(key_list[7], (HID,), jnp.float32), 0.1, 1.9),
        "out_proj": normal_values(key_list[8], (HID, C), HID ** -0.5, 0.5, ((1, 2),)),
    }


def layer_norm(values, gain):
    average = lax.optimization_barrier(jnp.mean(values, axis=0, keepdims=True))
    spread = lax.optimization_barrier(jnp.mean(jnp.square(values - average), axis=0, keepdims=True))
    return (values - average) * lax.rsqrt(spread + 1e-05) * gain[:, None, None]

def reference(pair_act, in_gain, left_proj, left_gate, right_proj, right_gate, out_gate, out_gain, out_proj):
    pair_float = pair_act.astype(jnp.float32)
    normed = layer_norm(pair_float, in_gain).astype(jnp.bfloat16)
    normed_float = normed.astype(jnp.float32)

    def lift_by(matrix):
        return jnp.einsum('cxy,ch->hxy', normed_float, matrix.astype(jnp.float32))
    left_edge = (jax.nn.sigmoid(lift_by(left_gate)) * lift_by(left_proj)).astype(jnp.bfloat16)
    right_edge = (jax.nn.sigmoid(lift_by(right_gate)) * lift_by(right_proj)).astype(jnp.bfloat16)
    gate_map = jax.nn.sigmoid(lift_by(out_gate))
    tri_sum = jnp.einsum('hki,hkj->hij', left_edge.astype(jnp.float32), right_edge.astype(jnp.float32))
    mid_norm = layer_norm(tri_sum, out_gain).astype(jnp.bfloat16)
    projected = jnp.einsum('hxy,hc->cxy', mid_norm.astype(jnp.float32), out_proj.astype(jnp.float32))
    return (gate_map * projected).astype(jnp.bfloat16)
```

```python
import functools

import jax
import jax.numpy as jnp
from jax import lax
from jax.experimental import pallas as pl
from jax.experimental.pallas import tpu as pltpu
from jax.sharding import PartitionSpec as P

MESH = pl.DeviceIdType.MESH
EPS = 1e-05
F32, BF16 = jnp.float32, jnp.bfloat16


def kernel(n, nx, pa, ing, lp, lg, rp, rg, og, outg, op, out,
           other, gains, gains_other, gain_all, x_all, wt, gate, y_left, y_right,
           send, recv, left_all, tri_send, tri_recv, tri_other,
           ready, ready_x, ch_send, ch_recv, z_send, z_recv, x_send, x_recv, t_send, t_recv):
    z, x, c = lax.axis_index("row"), lax.axis_index("col"), lax.axis_index("ch")
    ch, rows, lanes = pa.shape
    hp = ch // n
    bar = pltpu.get_barrier_semaphore()

    def each(lo, hi, f):
        def step(i, carry):
            f(i)
            return carry
        lax.fori_loop(lo, hi, step, 0)

    pl.semaphore_signal(bar, inc=1, device_id={"ch": 1 - c}, device_id_type=MESH)
    each(z + 1, n, lambda r: pl.semaphore_signal(bar, inc=1, device_id={"row": r}, device_id_type=MESH))
    each(0, x, lambda r: pl.semaphore_signal(bar, inc=1, device_id={"col": r}, device_id_type=MESH))
    pl.semaphore_wait(bar, z + (nx - 1 - x) + 1)
    each(0, z, lambda r: pl.semaphore_signal(ready.at[z], inc=1, device_id={"row": r}, device_id_type=MESH))
    each(x + 1, nx, lambda r: pl.semaphore_signal(ready_x.at[x], inc=1, device_id={"col": r}, device_id_type=MESH))

    def to_core(src, dst, i):
        return pltpu.make_async_remote_copy(src_ref=src, dst_ref=dst, send_sem=ch_send.at[i], recv_sem=ch_recv.at[i],
                                            device_id={"ch": 1 - c}, device_id_type=MESH)

    raw = to_core(pa, other, 0)
    raw.start()
    for i, g in enumerate((ing, outg)):
        gains[i] = jnp.broadcast_to(g[...], (lanes, ch)).T
    for i, w in enumerate((lp, lg, rp, rg, og)):
        wt[pl.ds(i * ch, ch), :] = w[...]
    gsent = to_core(gains, gains_other, 1)
    gsent.start()
    mine = pl.multiple_of(c * ch, ch)
    theirs = pl.multiple_of((1 - c) * ch, ch)
    gsent.wait_recv()
    for i in range(2):
        gain_all[i, pl.ds(mine, ch), :] = gains[i]
        gain_all[i, pl.ds(theirs, ch), :] = gains_other[i]
    raw.wait_recv()

    step_c = 8

    def layer_norm(a, b):
        def add(i, t):
            s = pl.ds(i * step_c, step_c)
            return t + a[s].astype(F32).sum(0) + b[s].astype(F32).sum(0)
        mean = lax.fori_loop(0, ch // step_c, add, jnp.zeros((rows, lanes), F32)) / (2 * ch)

        def sq(i, t):
            s = pl.ds(i * step_c, step_c)
            return t + jnp.square(a[s].astype(F32) - mean).sum(0) + jnp.square(b[s].astype(F32) - mean).sum(0)
        var = lax.fori_loop(0, ch // step_c, sq, jnp.zeros((rows, lanes), F32)) / (2 * ch)
        scale = lax.rsqrt(var + EPS)

        def put(i, carry):
            s = pl.ds(i * step_c, step_c)
            for r, base in ((a, mine), (b, theirs)):
                v = (r[s].astype(F32) - mean) * scale
                x_all[pl.ds(pl.multiple_of((base + i * step_c) * rows, rows * step_c), rows * step_c), :] = v.reshape(rows * step_c, lanes)
            return carry
        lax.fori_loop(0, ch // step_c, put, 0)

    layer_norm(pa, other)

    def lift(k):
        v = (x_all[pl.ds(k, 2 * ch, stride=rows), :] * gain_all[0]).astype(BF16)
        r = jnp.dot(wt[...], v, preferred_element_type=F32)
        y_left[pl.ds(k, ch, stride=rows), :] = jax.nn.sigmoid(r[ch : 2 * ch]) * r[:ch]
        y_right[pl.ds(k, ch, stride=rows), :] = jax.nn.sigmoid(r[3 * ch : 4 * ch]) * r[2 * ch : 3 * ch]
        gate[k] = jax.nn.sigmoid(r[4 * ch :])
    each(0, rows, lift)

    def pack(i):
        s = pl.ds(pl.multiple_of(i * hp * rows, hp * rows), hp * rows)
        send[i, 0] = y_left[s, :].reshape(hp, rows, lanes).astype(BF16)
        send[i, 1] = y_right[s, :].reshape(hp, rows, lanes).astype(BF16)
    each(0, n, pack)

    def to_row(r):
        pltpu.make_async_remote_copy(src_ref=send.at[r], dst_ref=recv.at[z], send_sem=z_send, recv_sem=z_recv.at[z],
                                     device_id={"row": r}, device_id_type=MESH).start()

    def down_half(i):
        d = n // 2 - i
        r1, r2 = lax.rem(z + d, n), lax.rem(z + n - d, n)

        @pl.when(r1 < z)
        def _():
            to_row(r1)

        @pl.when((r2 < z) & (d < n // 2))
        def _():
            to_row(r2)
    each(0, n // 2, down_half)
    recv[z] = send[z]

    def up(r):
        pl.semaphore_wait(ready.at[r], 1)
        to_row(r)
    each(z + 1, n, up)

    each(0, x, lambda r: pl.semaphore_wait(ready_x.at[r], 1))

    def to_col(s, r):
        return pltpu.make_async_remote_copy(src_ref=recv.at[s, 0], dst_ref=left_all.at[x, s], send_sem=x_send, recv_sem=x_recv.at[x],
                                            device_id={"col": r}, device_id_type=MESH)

    def spread(s):
        @pl.when(s != z)
        def _():
            pltpu.make_async_remote_copy(src_ref=send.at[s], dst_ref=recv.at[s], send_sem=z_send, recv_sem=z_recv.at[s],
                                         device_id={"row": s}, device_id_type=MESH).wait_recv()
        for d in range(1, nx):
            to_col(s, lax.rem(x + d, nx)).start()
        left_all[x, s] = recv[s, 0]
    each(0, n, spread)

    for d in range(1, nx):
        r = lax.rem(x + d, nx)
        pltpu.make_async_remote_copy(src_ref=left_all.at[r], dst_ref=left_all.at[r], send_sem=x_send, recv_sem=x_recv.at[r],
                                     device_id={"col": r}, device_id_type=MESH).wait_recv()

    per = lanes // rows
    for h in range(hp):
        right = recv[:, 1, h].reshape(n * rows, lanes)
        for q in range(nx):
            left = left_all[q, :, h].reshape(n * rows, lanes)
            t = lax.dot_general(left, right, (((0,), (0,)), ((), ())), preferred_element_type=F32)
            tri_send[pl.ds(q * per, per), h] = t.reshape(per, rows, lanes).astype(BF16)

    def tri_to(r):
        pltpu.make_async_remote_copy(src_ref=tri_send.at[r], dst_ref=tri_recv.at[z], send_sem=t_send, recv_sem=t_recv,
                                     device_id={"row": r}, device_id_type=MESH).start()

    def tri_out(i):
        d = n // 2 - i
        tri_to(lax.rem(z + d, n))

        @pl.when(d < n // 2)
        def _():
            tri_to(lax.rem(z + n - d, n))
    each(0, n // 2, tri_out)
    tri_recv[z] = tri_send[z]
    most = pl.ds(0, n - 1)
    pltpu.make_async_remote_copy(src_ref=tri_send.at[most], dst_ref=tri_recv.at[most], send_sem=t_send, recv_sem=t_recv,
                                 device_id={"row": lax.rem(z + 1, n)}, device_id_type=MESH).wait_recv()

    swap = to_core(tri_recv, tri_other, 2)
    swap.start()
    swap.wait_recv()
    layer_norm(tri_recv.reshape(ch, rows, lanes), tri_other.reshape(ch, rows, lanes))

    def close(k):
        v = (x_all[pl.ds(k, 2 * ch, stride=rows), :] * gain_all[1]).astype(BF16)
        y_left[pl.ds(k, ch, stride=rows), :] = jnp.dot(op[...], v, preferred_element_type=F32) * gate[k]
    each(0, rows, close)
    out[...] = y_left[...].reshape(ch, rows, lanes).astype(BF16)

    raw.wait_send()
    gsent.wait_send()
    swap.wait_send()
    pltpu.make_async_remote_copy(src_ref=send.at[most], dst_ref=recv.at[most], send_sem=z_send, recv_sem=z_recv.at[z],
                                 device_id={"row": lax.rem(z + 1, n)}, device_id_type=MESH).wait_send()
    pltpu.make_async_remote_copy(src_ref=tri_send.at[most], dst_ref=tri_recv.at[most], send_sem=t_send, recv_sem=t_recv,
                                 device_id={"row": lax.rem(z + 1, n)}, device_id_type=MESH).wait_send()
    for d in range(1, nx):
        r = lax.rem(x + d, nx)
        pltpu.make_async_remote_copy(src_ref=left_all.at[r], dst_ref=left_all.at[r], send_sem=x_send, recv_sem=x_recv.at[r],
                                     device_id={"col": r}, device_id_type=MESH).wait_send()


def solution(mesh):
    n, nx = mesh.shape["row"], mesh.shape["col"]

    def per_device(pair_act, in_gain, left_proj, left_gate, right_proj, right_gate, out_gate, out_gain, out_proj):
        ch, rows, lanes = pair_act.shape
        hp = ch // n
        vm = pltpu.VMEM
        dma, reg = pltpu.SemaphoreType.DMA, pltpu.SemaphoreType.REGULAR
        return pl.pallas_call(
            functools.partial(kernel, n, nx),
            out_shape=jax.ShapeDtypeStruct(pair_act.shape, BF16),
            in_specs=[pl.BlockSpec(memory_space=pltpu.VMEM)] * 9,
            out_specs=pl.BlockSpec(memory_space=pltpu.VMEM),
            scratch_shapes=[
                vm((ch, rows, lanes), BF16),
                vm((2, ch, lanes), F32),
                vm((2, ch, lanes), F32),
                vm((2, 2 * ch, lanes), F32),
                vm((2 * ch * rows, lanes), F32),
                vm((5 * ch, 2 * ch), BF16),
                vm((rows, ch, lanes), F32),
                vm((ch * rows, lanes), F32),
                vm((ch * rows, lanes), F32),
                vm((n, 2, hp, rows, lanes), BF16),
                vm((n, 2, hp, rows, lanes), BF16),
                vm((nx, n, hp, rows, lanes), BF16),
                vm((n, hp, rows, lanes), BF16),
                vm((n, hp, rows, lanes), BF16),
                vm((n, hp, rows, lanes), BF16),
                reg((n,)),
                reg((nx,)),
                dma((3,)),
                dma((3,)),
                dma,
                dma((n,)),
                dma,
                dma((nx,)),
                dma,
                dma,
            ],
            compiler_params=pltpu.CompilerParams(collective_id=0, has_side_effects=True),
            name="triangle",
        )(pair_act, in_gain[None], left_proj.T, left_gate.T, right_proj.T, right_gate.T, out_gate.T, out_gain[None], out_proj.T)

    return jax.shard_map(
        per_device,
        mesh=mesh,
        in_specs=(
            P("ch", ("grp", "row"), "col"),
            P("ch"),
            P(None, "ch"),
            P(None, "ch"),
            P(None, "ch"),
            P(None, "ch"),
            P(None, "ch"),
            P("ch"),
            P(None, "ch"),
        ),
        out_specs=P("ch", ("grp", "row"), "col"),
        check_vma=False,
    )
```

```python
import functools

import jax
import jax.numpy as jnp
from jax import lax
from jax.experimental import pallas as pl
from jax.experimental.pallas import tpu as pltpu
from jax.sharding import PartitionSpec as P

MESH = pl.DeviceIdType.MESH
EPS = 1e-05
GROUPS = 1
F32, BF16 = jnp.float32, jnp.bfloat16


def kernel(n, nx, pa_in, ing, lp, lg, rp, rg, og, outg, op, out,
           pa, other, rows_in, gains, gains_other, gain_all, x_all, v_all, wt, wo, gate, y,
           send, left_recv, right_recv, left_all, tri_send, tri_recv, tri_other,
           ready, ready_x, in_sem, ch_send, ch_recv, l_send, l_recv, r_send, r_recv, x_send, x_recv, t_send, t_recv, o_send, o_recv):
    z, x, c = lax.axis_index("row"), lax.axis_index("col"), lax.axis_index("ch")
    ch, rows, lanes = pa.shape
    hp = ch // n
    per_group = hp // GROUPS
    turn = lax.rem(z + n - 1, n)
    bar = pltpu.get_barrier_semaphore()

    def each(lo, hi, f, unroll=None):
        def step(i, carry):
            f(i)
            return carry
        lax.fori_loop(lo, hi, step, 0, unroll=unroll)

    def row_at(i):
        return lax.rem(i + 1, n)

    def turn_of(r):
        return lax.rem(r + n - 1, n)

    def to_core(src, dst, i):
        return pltpu.make_async_remote_copy(src_ref=src, dst_ref=dst, send_sem=ch_send.at[i], recv_sem=ch_recv.at[i],
                                            device_id={"ch": 1 - c}, device_id_type=MESH)

    pl.semaphore_signal(bar, inc=1, device_id={"ch": 1 - c}, device_id_type=MESH)
    loads = [pltpu.make_async_copy(pa_in, pa, in_sem.at[0]),
             pltpu.make_async_copy(ing, rows_in.at[0], in_sem.at[1]),
             pltpu.make_async_copy(outg, rows_in.at[1], in_sem.at[2])]
    for i, w in enumerate((lp, lg, rp, rg, og)):
        loads.append(pltpu.make_async_copy(w, wt.at[pl.ds(i * ch, ch), :], in_sem.at[3 + i]))
    loads.append(pltpu.make_async_copy(op, wo, in_sem.at[8]))
    for load in loads:
        load.start()
    each(0, x, lambda r: pl.semaphore_signal(bar, inc=1, device_id={"col": r}, device_id_type=MESH))
    each(turn + 1, n, lambda i: pl.semaphore_signal(bar, inc=1, device_id={"row": row_at(i)}, device_id_type=MESH))
    pl.semaphore_wait(bar, turn + (nx - 1 - x) + 1)
    raw = to_core(pa_in, other, 0)
    raw.start()
    each(0, turn, lambda i: pl.semaphore_signal(ready.at[z], inc=1, device_id={"row": row_at(i)}, device_id_type=MESH))
    each(x + 1, nx, lambda r: pl.semaphore_signal(ready_x.at[x], inc=1, device_id={"col": r}, device_id_type=MESH))
    for load in loads:
        load.wait()
    for i in range(2):
        gains[i] = jnp.broadcast_to(rows_in[i], (lanes, ch)).T
    gsent = to_core(gains, gains_other, 1)
    gsent.start()
    mine = pl.multiple_of(c * ch, ch)
    theirs = pl.multiple_of((1 - c) * ch, ch)
    raw.wait_recv()
    step_c = 8

    def layer_norm(a, b):
        def add(i, t):
            s = pl.ds(i * step_c, step_c)
            return t + a[s].astype(F32).sum(0) + b[s].astype(F32).sum(0)
        mean = lax.fori_loop(0, ch // step_c, add, jnp.zeros((rows, lanes), F32)) / (2 * ch)

        def sq(i, t):
            s = pl.ds(i * step_c, step_c)
            return t + jnp.square(a[s].astype(F32) - mean).sum(0) + jnp.square(b[s].astype(F32) - mean).sum(0)
        var = lax.fori_loop(0, ch // step_c, sq, jnp.zeros((rows, lanes), F32)) / (2 * ch)
        scale = lax.rsqrt(var + EPS)

        def put(i, carry):
            s = pl.ds(i * step_c, step_c)
            for r, base in ((a, mine), (b, theirs)):
                v = (r[s].astype(F32) - mean) * scale
                x_all[pl.ds(pl.multiple_of((base + i * step_c) * rows, rows * step_c), rows * step_c), :] = v.reshape(rows * step_c, lanes)
            return carry
        lax.fori_loop(0, ch // step_c, put, 0)

    layer_norm(pa, other)
    gsent.wait_recv()
    for i in range(2):
        gain_all[i, pl.ds(mine, ch), :] = gains[i]
        gain_all[i, pl.ds(theirs, ch), :] = gains_other[i]
    def edges(v, i):
        r = jnp.dot(wt[pl.ds(2 * i * ch, 2 * ch), :], v, preferred_element_type=F32)
        return jax.nn.sigmoid(r[ch:]) * r[:ch]

    def lift_left(k):
        v = (x_all[pl.ds(k, 2 * ch, stride=rows), :] * gain_all[0]).astype(BF16)
        v_all[k] = v
        y[pl.ds(k, ch, stride=rows), :] = edges(v, 0)
    each(0, rows, lift_left, 4)

    def pack(side):
        def one(i):
            s = pl.ds(pl.multiple_of(i * hp * rows, hp * rows), hp * rows)
            send[side, i] = y[s, :].reshape(hp, rows, lanes).astype(BF16)
        each(0, n, one, 4)
    pack(0)

    def part(g):
        return pl.ds(g * per_group, per_group)

    def left_copy(r, slot):
        return pltpu.make_async_remote_copy(src_ref=send.at[0, r], dst_ref=left_recv.at[slot], send_sem=l_send, recv_sem=l_recv.at[slot],
                                            device_id={"row": r}, device_id_type=MESH)

    def right_copy(h, r, slot):
        return pltpu.make_async_remote_copy(src_ref=send.at[1, r, part(h)], dst_ref=right_recv.at[h, slot], send_sem=r_send, recv_sem=r_recv.at[h],
                                            device_id={"row": r}, device_id_type=MESH)

    def down(copy):
        def one(i):
            d = n // 2 - i
            r1, r2 = lax.rem(z + d, n), lax.rem(z + n - d, n)

            @pl.when(turn_of(r1) < turn)
            def _():
                copy(r1, z).start()

            @pl.when((turn_of(r2) < turn) & (d < n // 2))
            def _():
                copy(r2, z).start()
        each(0, n // 2, one)
    down(left_copy)
    def lift_right(k):
        y[pl.ds(k, ch, stride=rows), :] = edges(v_all[k], 1)
    each(0, rows, lift_right, 4)
    pack(1)
    for h in range(GROUPS):
        down(functools.partial(right_copy, h))
    left_recv[z] = send[0, z]
    for h in range(GROUPS):
        right_recv[h, z] = send[1, z, h * per_group : (h + 1) * per_group]
    def lift_gate(k):
        gate[k] = jax.nn.sigmoid(jnp.dot(wt[pl.ds(4 * ch, ch), :], v_all[k], preferred_element_type=F32))
    each(0, rows, lift_gate, 4)
    def up_left(i):
        r = row_at(i)
        pl.semaphore_wait(ready.at[r], 1)
        left_copy(r, z).start()

    def up_right(h, i):
        right_copy(h, row_at(i), z).start()

    def up(i):
        up_left(i)
        for h in range(GROUPS):
            up_right(h, i)
    half = jnp.maximum(turn + 1, n // 2)
    each(turn + 1, half, up)
    each(half, n, up_left)
    for h in range(GROUPS):
        each(half, n, functools.partial(up_right, h))

    each(0, x, lambda r: pl.semaphore_wait(ready_x.at[r], 1))

    def to_col(s, r):
        return pltpu.make_async_remote_copy(src_ref=left_recv.at[s], dst_ref=left_all.at[x, s], send_sem=x_send, recv_sem=x_recv.at[x],
                                            device_id={"col": r}, device_id_type=MESH)

    def spread(s):
        @pl.when(s != z)
        def _():
            left_copy(s, s).wait_recv()
        for d in range(1, nx):
            to_col(s, lax.rem(x + d, nx)).start()
        left_all[x, s] = left_recv[s]
    each(0, n, lambda i: spread(row_at(i)))

    def all_rows(src, dst, ss, rs):
        most = pl.ds(0, n - 1)
        return pltpu.make_async_remote_copy(src_ref=src.at[most], dst_ref=dst.at[most], send_sem=ss, recv_sem=rs,
                                            device_id={"row": lax.rem(z + 1, n)}, device_id_type=MESH)

    def whole_col(d):
        r = lax.rem(x + d, nx)
        return pltpu.make_async_remote_copy(src_ref=left_all.at[r], dst_ref=left_all.at[r], send_sem=x_send, recv_sem=x_recv.at[r],
                                            device_id={"col": r}, device_id_type=MESH)
    for d in range(1, nx):
        whole_col(d).wait_recv()
    def tri_copy(h, r, slot):
        return pltpu.make_async_remote_copy(src_ref=tri_send.at[h, r], dst_ref=tri_recv.at[slot, part(h)], send_sem=t_send, recv_sem=t_recv.at[h, slot],
                                            device_id={"row": r}, device_id_type=MESH)

    def swap(h, s):
        return pltpu.make_async_remote_copy(src_ref=tri_recv.at[s, part(h)], dst_ref=tri_other.at[s, part(h)], send_sem=o_send, recv_sem=o_recv,
                                            device_id={"ch": 1 - c}, device_id_type=MESH)

    per = lanes // rows
    for h in range(GROUPS):
        all_rows(right_recv.at[h], right_recv.at[h], r_send, r_recv.at[h]).wait_recv()
        for m in range(per_group):
            right = right_recv[h, :, m].reshape(n * rows, lanes)
            for q in range(nx):
                left = left_all[q, :, h * per_group + m].reshape(n * rows, lanes)
                t = lax.dot_general(left, right, (((0,), (0,)), ((), ())), preferred_element_type=F32)
                tri_send[h, pl.ds(q * per, per), m] = t.reshape(per, rows, lanes).astype(BF16)

        def tri_out(i):
            d = n // 2 - i
            tri_copy(h, lax.rem(z + d, n), z).start()

            @pl.when(d < n // 2)
            def _():
                tri_copy(h, lax.rem(z + n - d, n), z).start()
        each(0, n // 2, tri_out)
        tri_recv[z, h * per_group : (h + 1) * per_group] = tri_send[h, z]

    for h in range(GROUPS):
        swap(h, z).start()

        def tri_in(i):
            d = n // 2 - i
            r1, r2 = lax.rem(z + d, n), lax.rem(z + n - d, n)
            tri_copy(h, r1, r1).wait_recv()
            swap(h, r1).start()

            @pl.when(d < n // 2)
            def _():
                tri_copy(h, r2, r2).wait_recv()
                swap(h, r2).start()
        each(0, n // 2, tri_in)
    swapped = pltpu.make_async_remote_copy(src_ref=tri_recv, dst_ref=tri_other, send_sem=o_send, recv_sem=o_recv,
                                           device_id={"ch": 1 - c}, device_id_type=MESH)
    swapped.wait_recv()
    layer_norm(tri_recv.reshape(ch, rows, lanes), tri_other.reshape(ch, rows, lanes))

    def close(k):
        v = (x_all[pl.ds(k, 2 * ch, stride=rows), :] * gain_all[1]).astype(BF16)
        y[pl.ds(k, ch, stride=rows), :] = jnp.dot(wo[...], v, preferred_element_type=F32) * gate[k]
    each(0, rows, close, 4)
    out[...] = y[...].reshape(ch, rows, lanes).astype(BF16)

    raw.wait_send()
    gsent.wait_send()
    swapped.wait_send()
    all_rows(send.at[0], left_recv, l_send, r_recv.at[0]).wait_send()
    for h in range(GROUPS):
        all_rows(right_recv.at[h], right_recv.at[h], r_send, r_recv.at[h]).wait_send()
        all_rows(tri_send.at[h], tri_send.at[h], t_send, r_recv.at[h]).wait_send()
    for d in range(1, nx):
        whole_col(d).wait_send()


def solution(mesh):
    n, nx = mesh.shape["row"], mesh.shape["col"]

    def per_device(pair_act, in_gain, left_proj, left_gate, right_proj, right_gate, out_gate, out_gain, out_proj):
        ch, rows, lanes = pair_act.shape
        hp = ch // n
        vm = pltpu.VMEM
        dma, reg = pltpu.SemaphoreType.DMA, pltpu.SemaphoreType.REGULAR
        return pl.pallas_call(
            functools.partial(kernel, n, nx),
            out_shape=jax.ShapeDtypeStruct(pair_act.shape, BF16),
            in_specs=[pl.BlockSpec(memory_space=pl.ANY)] * 9,
            out_specs=pl.BlockSpec(memory_space=pltpu.VMEM),
            scratch_shapes=[
                vm((ch, rows, lanes), BF16),
                vm((ch, rows, lanes), BF16),
                vm((2, 1, ch), F32),
                vm((2, ch, lanes), F32),
                vm((2, ch, lanes), F32),
                vm((2, 2 * ch, lanes), F32),
                vm((2 * ch * rows, lanes), F32),
                vm((rows, 2 * ch, lanes), BF16),
                vm((5 * ch, 2 * ch), BF16),
                vm((ch, 2 * ch), BF16),
                vm((rows, ch, lanes), F32),
                vm((ch * rows, lanes), F32),
                vm((2, n, hp, rows, lanes), BF16),
                vm((n, hp, rows, lanes), BF16),
                vm((GROUPS, n, hp // GROUPS, rows, lanes), BF16),
                vm((nx, n, hp, rows, lanes), BF16),
                vm((GROUPS, n, hp // GROUPS, rows, lanes), BF16),
                vm((n, hp, rows, lanes), BF16),
                vm((n, hp, rows, lanes), BF16),
                reg((n,)),
                reg((nx,)),
                dma((9,)),
                dma((2,)),
                dma((2,)),
                dma,
                dma((n,)),
                dma,
                dma((GROUPS,)),
                dma,
                dma((nx,)),
                dma,
                dma((GROUPS, n)),
                dma,
                dma,
            ],
            compiler_params=pltpu.CompilerParams(collective_id=0, has_side_effects=True),
            name="triangle",
        )(pair_act, in_gain[None], left_proj.T, left_gate.T, right_proj.T, right_gate.T, out_gate.T, out_gain[None], out_proj.T)

    return jax.shard_map(
        per_device,
        mesh=mesh,
        in_specs=(
            P("ch", ("grp", "row"), "col"),
            P("ch"),
            P(None, "ch"),
            P(None, "ch"),
            P(None, "ch"),
            P(None, "ch"),
            P(None, "ch"),
            P("ch"),
            P(None, "ch"),
        ),
        out_specs=P("ch", ("grp", "row"), "col"),
        check_vma=False,
    )
```

```python
import functools

import jax
import jax.numpy as jnp
from jax import lax
from jax.experimental import pallas as pl
from jax.experimental.pallas import tpu as pltpu
from jax.sharding import PartitionSpec as P

MESH = pl.DeviceIdType.MESH
EPS = 1e-05
GROUPS = 1
F32, BF16 = jnp.float32, jnp.bfloat16


def kernel(n, nx, pa_in, ing, lp, lg, rp, rg, og, outg, op, out,
           pa, other, rows_in, gains, gains_other, gain_all, x_all, v_all, wt, wo, gate, y,
           send, left_recv, right_recv, left_all, tri_send, tri_recv, tri_other,
           ready, ready_x, in_sem, ch_send, ch_recv, l_send, l_recv, r_send, r_recv, x_send, x_recv, t_send, t_recv, o_send, o_recv):
    z, x, c = lax.axis_index("row"), lax.axis_index("col"), lax.axis_index("ch")
    ch, rows, lanes = pa.shape
    hp = ch // n
    per_group = hp // GROUPS
    turn = lax.rem(z + n - 1, n)
    bar = pltpu.get_barrier_semaphore()

    def each(lo, hi, f, unroll=None):
        def step(i, carry):
            f(i)
            return carry
        lax.fori_loop(lo, hi, step, 0, unroll=unroll)

    def row_at(i):
        return lax.rem(i + 1, n)

    def turn_of(r):
        return lax.rem(r + n - 1, n)

    def to_core(src, dst, i):
        return pltpu.make_async_remote_copy(src_ref=src, dst_ref=dst, send_sem=ch_send.at[i], recv_sem=ch_recv.at[i],
                                            device_id={"ch": 1 - c}, device_id_type=MESH)

    pl.semaphore_signal(bar, inc=1, device_id={"ch": 1 - c}, device_id_type=MESH)
    loads = [pltpu.make_async_copy(pa_in, pa, in_sem.at[0]),
             pltpu.make_async_copy(ing, rows_in.at[0], in_sem.at[1]),
             pltpu.make_async_copy(outg, rows_in.at[1], in_sem.at[2])]
    for i, w in enumerate((lp, lg, rp, rg, og)):
        loads.append(pltpu.make_async_copy(w, wt.at[pl.ds(i * ch, ch), :], in_sem.at[3 + i]))
    loads.append(pltpu.make_async_copy(op, wo, in_sem.at[8]))
    for load in loads:
        load.start()
    each(0, x, lambda r: pl.semaphore_signal(bar, inc=1, device_id={"col": r}, device_id_type=MESH))
    each(turn + 1, n, lambda i: pl.semaphore_signal(bar, inc=1, device_id={"row": row_at(i)}, device_id_type=MESH))
    pl.semaphore_wait(bar, turn + (nx - 1 - x) + 1)
    raw = to_core(pa_in, other, 0)
    raw.start()
    each(0, turn, lambda i: pl.semaphore_signal(ready.at[z], inc=1, device_id={"row": row_at(i)}, device_id_type=MESH))
    each(x + 1, nx, lambda r: pl.semaphore_signal(ready_x.at[x], inc=1, device_id={"col": r}, device_id_type=MESH))
    for load in loads:
        load.wait()
    for i in range(2):
        gains[i] = jnp.broadcast_to(rows_in[i], (lanes, ch)).T
    gsent = to_core(gains, gains_other, 1)
    gsent.start()
    mine = pl.multiple_of(c * ch, ch)
    theirs = pl.multiple_of((1 - c) * ch, ch)
    raw.wait_recv()
    step_c = 8

    def layer_norm(a, b):
        def add(i, t):
            s = pl.ds(i * step_c, step_c)
            return t + a[s].astype(F32).sum(0) + b[s].astype(F32).sum(0)
        mean = lax.fori_loop(0, ch // step_c, add, jnp.zeros((rows, lanes), F32)) / (2 * ch)

        def sq(i, t):
            s = pl.ds(i * step_c, step_c)
            return t + jnp.square(a[s].astype(F32) - mean).sum(0) + jnp.square(b[s].astype(F32) - mean).sum(0)
        var = lax.fori_loop(0, ch // step_c, sq, jnp.zeros((rows, lanes), F32)) / (2 * ch)
        scale = lax.rsqrt(var + EPS)

        def put(i, carry):
            s = pl.ds(i * step_c, step_c)
            for r, base in ((a, mine), (b, theirs)):
                v = (r[s].astype(F32) - mean) * scale
                x_all[pl.ds(pl.multiple_of((base + i * step_c) * rows, rows * step_c), rows * step_c), :] = v.reshape(rows * step_c, lanes)
            return carry
        lax.fori_loop(0, ch // step_c, put, 0)

    layer_norm(pa, other)
    gsent.wait_recv()
    for i in range(2):
        gain_all[i, pl.ds(mine, ch), :] = gains[i]
        gain_all[i, pl.ds(theirs, ch), :] = gains_other[i]
    def edges(v, i):
        r = jnp.dot(wt[pl.ds(2 * i * ch, 2 * ch), :], v, preferred_element_type=F32)
        return jax.nn.sigmoid(r[ch:]) * r[:ch]

    def lift_left(k):
        v = (x_all[pl.ds(k, 2 * ch, stride=rows), :] * gain_all[0]).astype(BF16)
        v_all[k] = v
        y[pl.ds(k, ch, stride=rows), :] = edges(v, 0)
    each(0, rows, lift_left, 4)

    def pack(side):
        def one(i):
            s = pl.ds(pl.multiple_of(i * hp * rows, hp * rows), hp * rows)
            send[side, i] = y[s, :].reshape(hp, rows, lanes).astype(BF16)
        each(0, n, one, 4)
    pack(0)

    def part(g):
        return pl.ds(g * per_group, per_group)

    def left_copy(r, slot):
        return pltpu.make_async_remote_copy(src_ref=send.at[0, r], dst_ref=left_recv.at[slot], send_sem=l_send, recv_sem=l_recv.at[slot],
                                            device_id={"row": r}, device_id_type=MESH)

    def right_copy(h, r, slot):
        return pltpu.make_async_remote_copy(src_ref=send.at[1, r, part(h)], dst_ref=right_recv.at[h, slot], send_sem=r_send, recv_sem=r_recv.at[h],
                                            device_id={"row": r}, device_id_type=MESH)

    def down_at(copy, i):
        d = n // 2 - i
        r1, r2 = lax.rem(z + d, n), lax.rem(z + n - d, n)

        @pl.when(turn_of(r1) < turn)
        def _():
            copy(r1, z).start()

        @pl.when((turn_of(r2) < turn) & (d < n // 2))
        def _():
            copy(r2, z).start()
    each(0, n // 2, functools.partial(down_at, left_copy))
    def lift_right(k):
        y[pl.ds(k, ch, stride=rows), :] = edges(v_all[k], 1)
    each(0, rows, lift_right, 4)
    pack(1)
    for h in range(GROUPS):
        right_recv[h, z] = send[1, z, h * per_group : (h + 1) * per_group]
    left_recv[z] = send[0, z]

    def down_right(i):
        for h in range(GROUPS):
            down_at(functools.partial(right_copy, h), i)

    def up_left(i):
        r = row_at(i)
        pl.semaphore_wait(ready.at[r], 1)
        left_copy(r, z).start()

    def up_right(i):
        for h in range(GROUPS):
            right_copy(h, row_at(i), z).start()

    def up(i):
        up_left(i)
        up_right(i)
    early = turn < n // 2
    ahead = jnp.where(early, n // 2, 0)
    each(0, ahead, down_right)
    half = jnp.maximum(turn + 1, n // 2)
    each(turn + 1, half, up)

    def mixed(i):
        up_left(i)
        t = ahead + i - turn - 1

        @pl.when(t < n // 2)
        def _():
            down_right(t)
    each(half, n, mixed)
    each(jnp.minimum(ahead + n - half, n // 2), n // 2, down_right)
    each(half, n, up_right)
    def lift_gate(k):
        gate[k] = jax.nn.sigmoid(jnp.dot(wt[pl.ds(4 * ch, ch), :], v_all[k], preferred_element_type=F32))
    each(0, rows, lift_gate, 4)
    each(0, x, lambda r: pl.semaphore_wait(ready_x.at[r], 1))

    def to_col(s, r):
        return pltpu.make_async_remote_copy(src_ref=left_recv.at[s], dst_ref=left_all.at[x, s], send_sem=x_send, recv_sem=x_recv.at[x],
                                            device_id={"col": r}, device_id_type=MESH)

    def spread(s):
        @pl.when(s != z)
        def _():
            left_copy(s, s).wait_recv()
        for d in range(1, nx):
            to_col(s, lax.rem(x + d, nx)).start()
        left_all[x, s] = left_recv[s]
    each(0, n, lambda i: spread(row_at(i)))

    def all_rows(src, dst, ss, rs):
        most = pl.ds(0, n - 1)
        return pltpu.make_async_remote_copy(src_ref=src.at[most], dst_ref=dst.at[most], send_sem=ss, recv_sem=rs,
                                            device_id={"row": lax.rem(z + 1, n)}, device_id_type=MESH)

    def whole_col(d):
        r = lax.rem(x + d, nx)
        return pltpu.make_async_remote_copy(src_ref=left_all.at[r], dst_ref=left_all.at[r], send_sem=x_send, recv_sem=x_recv.at[r],
                                            device_id={"col": r}, device_id_type=MESH)
    for d in range(1, nx):
        whole_col(d).wait_recv()
    def tri_copy(h, r, slot):
        return pltpu.make_async_remote_copy(src_ref=tri_send.at[h, r], dst_ref=tri_recv.at[slot, part(h)], send_sem=t_send, recv_sem=t_recv.at[h, slot],
                                            device_id={"row": r}, device_id_type=MESH)

    def swap(h, s):
        return pltpu.make_async_remote_copy(src_ref=tri_recv.at[s, part(h)], dst_ref=tri_other.at[s, part(h)], send_sem=o_send, recv_sem=o_recv,
                                            device_id={"ch": 1 - c}, device_id_type=MESH)

    per = lanes // rows
    for h in range(GROUPS):
        all_rows(right_recv.at[h], right_recv.at[h], r_send, r_recv.at[h]).wait_recv()
        for m in range(per_group):
            right = right_recv[h, :, m].reshape(n * rows, lanes)
            for q in range(nx):
                left = left_all[q, :, h * per_group + m].reshape(n * rows, lanes)
                t = lax.dot_general(left, right, (((0,), (0,)), ((), ())), preferred_element_type=F32)
                tri_send[h, pl.ds(q * per, per), m] = t.reshape(per, rows, lanes).astype(BF16)

        def tri_out(i):
            d = n // 2 - i
            tri_copy(h, lax.rem(z + d, n), z).start()

            @pl.when(d < n // 2)
            def _():
                tri_copy(h, lax.rem(z + n - d, n), z).start()
        each(0, n // 2, tri_out)
        tri_recv[z, h * per_group : (h + 1) * per_group] = tri_send[h, z]

    for h in range(GROUPS):
        swap(h, z).start()

        def tri_in(i):
            d = n // 2 - i
            r1, r2 = lax.rem(z + d, n), lax.rem(z + n - d, n)
            tri_copy(h, r1, r1).wait_recv()
            swap(h, r1).start()

            @pl.when(d < n // 2)
            def _():
                tri_copy(h, r2, r2).wait_recv()
                swap(h, r2).start()
        each(0, n // 2, tri_in)
    swapped = pltpu.make_async_remote_copy(src_ref=tri_recv, dst_ref=tri_other, send_sem=o_send, recv_sem=o_recv,
                                           device_id={"ch": 1 - c}, device_id_type=MESH)
    swapped.wait_recv()
    layer_norm(tri_recv.reshape(ch, rows, lanes), tri_other.reshape(ch, rows, lanes))

    def close(k):
        v = (x_all[pl.ds(k, 2 * ch, stride=rows), :] * gain_all[1]).astype(BF16)
        y[pl.ds(k, ch, stride=rows), :] = jnp.dot(wo[...], v, preferred_element_type=F32) * gate[k]
    each(0, rows, close, 4)
    out[...] = y[...].reshape(ch, rows, lanes).astype(BF16)

    raw.wait_send()
    gsent.wait_send()
    swapped.wait_send()
    all_rows(send.at[0], left_recv, l_send, r_recv.at[0]).wait_send()
    for h in range(GROUPS):
        all_rows(right_recv.at[h], right_recv.at[h], r_send, r_recv.at[h]).wait_send()
        all_rows(tri_send.at[h], tri_send.at[h], t_send, r_recv.at[h]).wait_send()
    for d in range(1, nx):
        whole_col(d).wait_send()


def solution(mesh):
    n, nx = mesh.shape["row"], mesh.shape["col"]

    def per_device(pair_act, in_gain, left_proj, left_gate, right_proj, right_gate, out_gate, out_gain, out_proj):
        ch, rows, lanes = pair_act.shape
        hp = ch // n
        vm = pltpu.VMEM
        dma, reg = pltpu.SemaphoreType.DMA, pltpu.SemaphoreType.REGULAR
        return pl.pallas_call(
            functools.partial(kernel, n, nx),
            out_shape=pltpu.VMEM(pair_act.shape, BF16),
            in_specs=[pl.BlockSpec(memory_space=pl.ANY)] * 9,
            out_specs=pl.BlockSpec(memory_space=pltpu.VMEM),
            scratch_shapes=[
                vm((ch, rows, lanes), BF16),
                vm((ch, rows, lanes), BF16),
                vm((2, 1, ch), F32),
                vm((2, ch, lanes), F32),
                vm((2, ch, lanes), F32),
                vm((2, 2 * ch, lanes), F32),
                vm((2 * ch * rows, lanes), F32),
                vm((rows, 2 * ch, lanes), BF16),
                vm((5 * ch, 2 * ch), BF16),
                vm((ch, 2 * ch), BF16),
                vm((rows, ch, lanes), F32),
                vm((ch * rows, lanes), F32),
                vm((2, n, hp, rows, lanes), BF16),
                vm((n, hp, rows, lanes), BF16),
                vm((GROUPS, n, hp // GROUPS, rows, lanes), BF16),
                vm((nx, n, hp, rows, lanes), BF16),
                vm((GROUPS, n, hp // GROUPS, rows, lanes), BF16),
                vm((n, hp, rows, lanes), BF16),
                vm((n, hp, rows, lanes), BF16),
                reg((n,)),
                reg((nx,)),
                dma((9,)),
                dma((2,)),
                dma((2,)),
                dma,
                dma((n,)),
                dma,
                dma((GROUPS,)),
                dma,
                dma((nx,)),
                dma,
                dma((GROUPS, n)),
                dma,
                dma,
            ],
            compiler_params=pltpu.CompilerParams(collective_id=0, has_side_effects=True),
            name="triangle",
        )(pair_act, in_gain[None], left_proj.T, left_gate.T, right_proj.T, right_gate.T, out_gate.T, out_gain[None], out_proj.T)

    return jax.shard_map(
        per_device,
        mesh=mesh,
        in_specs=(
            P("ch", ("grp", "row"), "col"),
            P("ch"),
            P(None, "ch"),
            P(None, "ch"),
            P(None, "ch"),
            P(None, "ch"),
            P(None, "ch"),
            P("ch"),
            P(None, "ch"),
        ),
        out_specs=P("ch", ("grp", "row"), "col"),
        check_vma=False,
    )
```

```python
import functools

import jax
import jax.numpy as jnp
from jax import lax
from jax.experimental import pallas as pl
from jax.experimental.pallas import tpu as pltpu
from jax.sharding import PartitionSpec as P

MESH = pl.DeviceIdType.MESH
EPS = 1e-05
GROUPS = 1
F32, BF16 = jnp.float32, jnp.bfloat16


def kernel(n, nx, pa_in, ing, lp, lg, rp, rg, og, outg, op, out,
           pa, other, rows_in, gains, gains_other, gain_all, x_all, v_all, wt, wo, gate, y,
           send, left_recv, right_recv, left_all, tri_send, tri_recv, tri_other,
           ready, ready_x, in_sem, ch_send, ch_recv, l_send, l_recv, r_send, r_recv, x_send, x_recv, t_send, t_recv, o_send, o_recv):
    z, x, c = lax.axis_index("row"), lax.axis_index("col"), lax.axis_index("ch")
    ch, rows, lanes = pa.shape
    hp = ch // n
    per_group = hp // GROUPS
    turn = lax.rem(z + n - 1, n)
    bar = pltpu.get_barrier_semaphore()

    def each(lo, hi, f, unroll=None):
        def step(i, carry):
            f(i)
            return carry
        lax.fori_loop(lo, hi, step, 0, unroll=unroll)

    def row_at(i):
        return lax.rem(i + 1, n)

    def turn_of(r):
        return lax.rem(r + n - 1, n)

    def to_core(src, dst, i):
        return pltpu.make_async_remote_copy(src_ref=src, dst_ref=dst, send_sem=ch_send.at[i], recv_sem=ch_recv.at[i],
                                            device_id={"ch": 1 - c}, device_id_type=MESH)

    pl.semaphore_signal(bar, inc=1, device_id={"ch": 1 - c}, device_id_type=MESH)
    loads = [pltpu.make_async_copy(pa_in, pa, in_sem.at[0]),
             pltpu.make_async_copy(ing, rows_in.at[0], in_sem.at[1]),
             pltpu.make_async_copy(outg, rows_in.at[1], in_sem.at[2])]
    for i, w in enumerate((lp, lg, rp, rg, og)):
        loads.append(pltpu.make_async_copy(w, wt.at[pl.ds(i * ch, ch), :], in_sem.at[3 + i]))
    loads.append(pltpu.make_async_copy(op, wo, in_sem.at[8]))
    for load in loads:
        load.start()
    each(0, x, lambda r: pl.semaphore_signal(bar, inc=1, device_id={"col": r}, device_id_type=MESH))
    each(turn + 1, n, lambda i: pl.semaphore_signal(bar, inc=1, device_id={"row": row_at(i)}, device_id_type=MESH))
    pl.semaphore_wait(bar, turn + (nx - 1 - x) + 1)
    raw = to_core(pa, other, 0)
    loads[0].wait()
    raw.start()
    each(0, turn, lambda i: pl.semaphore_signal(ready.at[z], inc=1, device_id={"row": row_at(i)}, device_id_type=MESH))
    each(x + 1, nx, lambda r: pl.semaphore_signal(ready_x.at[x], inc=1, device_id={"col": r}, device_id_type=MESH))
    for load in loads[1:]:
        load.wait()
    for i in range(2):
        gains[i] = jnp.broadcast_to(rows_in[i], (lanes, ch)).T
    gsent = to_core(gains, gains_other, 1)
    gsent.start()
    mine = pl.multiple_of(c * ch, ch)
    theirs = pl.multiple_of((1 - c) * ch, ch)
    raw.wait_recv()
    step_c = 8

    def layer_norm(a, b):
        def add(i, t):
            s = pl.ds(i * step_c, step_c)
            return t + a[s].astype(F32).sum(0) + b[s].astype(F32).sum(0)
        mean = lax.fori_loop(0, ch // step_c, add, jnp.zeros((rows, lanes), F32)) / (2 * ch)

        def sq(i, t):
            s = pl.ds(i * step_c, step_c)
            return t + jnp.square(a[s].astype(F32) - mean).sum(0) + jnp.square(b[s].astype(F32) - mean).sum(0)
        var = lax.fori_loop(0, ch // step_c, sq, jnp.zeros((rows, lanes), F32)) / (2 * ch)
        scale = lax.rsqrt(var + EPS)

        def put(i, carry):
            s = pl.ds(i * step_c, step_c)
            for r, base in ((a, mine), (b, theirs)):
                v = (r[s].astype(F32) - mean) * scale
                x_all[pl.ds(pl.multiple_of((base + i * step_c) * rows, rows * step_c), rows * step_c), :] = v.reshape(rows * step_c, lanes)
            return carry
        lax.fori_loop(0, ch // step_c, put, 0)

    layer_norm(pa, other)
    gsent.wait_recv()
    for i in range(2):
        gain_all[i, pl.ds(mine, ch), :] = gains[i]
        gain_all[i, pl.ds(theirs, ch), :] = gains_other[i]
    def edges(v, i):
        r = jnp.dot(wt[pl.ds(2 * i * ch, 2 * ch), :], v, preferred_element_type=F32)
        return jax.nn.sigmoid(r[ch:]) * r[:ch]

    def lift_left(k):
        v = (x_all[pl.ds(k, 2 * ch, stride=rows), :] * gain_all[0]).astype(BF16)
        v_all[k] = v
        y[pl.ds(k, ch, stride=rows), :] = edges(v, 0)
    each(0, rows, lift_left, 8)

    def pack(side):
        def one(i):
            s = pl.ds(pl.multiple_of(i * hp * rows, hp * rows), hp * rows)
            send[side, i] = y[s, :].reshape(hp, rows, lanes).astype(BF16)
        each(0, n, one, 4)
    pack(0)

    def part(g):
        return pl.ds(g * per_group, per_group)

    def left_copy(r, slot):
        return pltpu.make_async_remote_copy(src_ref=send.at[0, r], dst_ref=left_recv.at[slot], send_sem=l_send, recv_sem=l_recv.at[slot],
                                            device_id={"row": r}, device_id_type=MESH)

    def right_copy(h, r, slot):
        return pltpu.make_async_remote_copy(src_ref=send.at[1, r, part(h)], dst_ref=right_recv.at[h, slot], send_sem=r_send, recv_sem=r_recv.at[h],
                                            device_id={"row": r}, device_id_type=MESH)

    def down_at(copy, i):
        d = n // 2 - i
        r1, r2 = lax.rem(z + d, n), lax.rem(z + n - d, n)

        @pl.when(turn_of(r1) < turn)
        def _():
            copy(r1, z).start()

        @pl.when((turn_of(r2) < turn) & (d < n // 2))
        def _():
            copy(r2, z).start()
    each(0, n // 2, functools.partial(down_at, left_copy))
    def lift_right(k):
        y[pl.ds(k, ch, stride=rows), :] = edges(v_all[k], 1)
    each(0, rows, lift_right, 4)
    pack(1)
    for h in range(GROUPS):
        right_recv[h, z] = send[1, z, h * per_group : (h + 1) * per_group]
    left_recv[z] = send[0, z]

    def down_right(i):
        for h in range(GROUPS):
            down_at(functools.partial(right_copy, h), i)

    def up_left(i):
        r = row_at(i)
        pl.semaphore_wait(ready.at[r], 1)
        left_copy(r, z).start()

    def up_right(i):
        for h in range(GROUPS):
            right_copy(h, row_at(i), z).start()

    def up(i):
        up_left(i)
        up_right(i)
    early = turn < n // 2
    ahead = jnp.where(early, n // 2, 0)
    each(0, ahead, down_right)
    half = jnp.maximum(turn + 1, n // 2)
    each(turn + 1, half, up)

    def mixed(i):
        up_left(i)
        t = ahead + i - turn - 1

        @pl.when(t < n // 2)
        def _():
            down_right(t)
    each(half, n, mixed)
    each(jnp.minimum(ahead + n - half, n // 2), n // 2, down_right)
    each(half, n, up_right)
    def lift_gate(k):
        gate[k] = jax.nn.sigmoid(jnp.dot(wt[pl.ds(4 * ch, ch), :], v_all[k], preferred_element_type=F32))
    each(0, rows, lift_gate, 4)
    each(0, x, lambda r: pl.semaphore_wait(ready_x.at[r], 1))

    def to_col(s, r):
        return pltpu.make_async_remote_copy(src_ref=left_recv.at[s], dst_ref=left_all.at[x, s], send_sem=x_send, recv_sem=x_recv.at[x],
                                            device_id={"col": r}, device_id_type=MESH)

    def spread(s):
        for d in range(1, nx):
            to_col(s, lax.rem(x + d, nx)).start()
        left_all[x, s] = left_recv[s]

    def arrived(s):
        left_copy(s, s).wait_recv()
        spread(s)
    spread(z)

    last = turn >= n - n // 4

    def in_order(i):
        @pl.when(i != turn)
        def _():
            arrived(row_at(i))
    each(0, jnp.where(last, 0, n), in_order)

    def farthest(i):
        d = n // 2 - i
        arrived(lax.rem(z + d, n))

        @pl.when(d < n // 2)
        def _():
            arrived(lax.rem(z + n - d, n))
    each(jnp.where(last, 0, n // 2), n // 2, farthest)

    def all_rows(src, dst, ss, rs):
        most = pl.ds(0, n - 1)
        return pltpu.make_async_remote_copy(src_ref=src.at[most], dst_ref=dst.at[most], send_sem=ss, recv_sem=rs,
                                            device_id={"row": lax.rem(z + 1, n)}, device_id_type=MESH)

    def whole_col(d):
        r = lax.rem(x + d, nx)
        return pltpu.make_async_remote_copy(src_ref=left_all.at[r], dst_ref=left_all.at[r], send_sem=x_send, recv_sem=x_recv.at[r],
                                            device_id={"col": r}, device_id_type=MESH)
    for d in range(1, nx):
        whole_col(d).wait_recv()
    def tri_copy(h, r, slot):
        return pltpu.make_async_remote_copy(src_ref=tri_send.at[h, r], dst_ref=tri_recv.at[slot, part(h)], send_sem=t_send, recv_sem=t_recv.at[h, slot],
                                            device_id={"row": r}, device_id_type=MESH)

    def swap(h, s):
        return pltpu.make_async_remote_copy(src_ref=tri_recv.at[s, part(h)], dst_ref=tri_other.at[s, part(h)], send_sem=o_send, recv_sem=o_recv,
                                            device_id={"ch": 1 - c}, device_id_type=MESH)

    per = lanes // rows
    for h in range(GROUPS):
        all_rows(right_recv.at[h], right_recv.at[h], r_send, r_recv.at[h]).wait_recv()
        rights = [right_recv[h, :, m].reshape(n * rows, lanes) for m in range(per_group)]

        def tri_block(q):
            for m in range(per_group):
                left = left_all[q, :, h * per_group + m].reshape(n * rows, lanes)
                t = lax.dot_general(left, rights[m], (((0,), (0,)), ((), ())), preferred_element_type=F32)
                tri_send[h, pl.ds(pl.multiple_of(q * per, per), per), m] = t.reshape(per, rows, lanes).astype(BF16)

        def tri_to(r):
            @pl.when(r != z)
            def _():
                tri_copy(h, r, z).start()

        def far_block(i):
            q = lax.rem(z // per + nx // 2 + i, nx)
            tri_block(q)
            each(0, per, lambda k: tri_to(q * per + k))
        each(0, nx, far_block)
        tri_recv[z, h * per_group : (h + 1) * per_group] = tri_send[h, z]

    for h in range(GROUPS):
        swap(h, z).start()

        def tri_in(i):
            d = n // 2 - i
            r1, r2 = lax.rem(z + d, n), lax.rem(z + n - d, n)
            tri_copy(h, r1, r1).wait_recv()
            swap(h, r1).start()

            @pl.when(d < n // 2)
            def _():
                tri_copy(h, r2, r2).wait_recv()
                swap(h, r2).start()
        each(0, n // 2, tri_in)
    swapped = pltpu.make_async_remote_copy(src_ref=tri_recv, dst_ref=tri_other, send_sem=o_send, recv_sem=o_recv,
                                           device_id={"ch": 1 - c}, device_id_type=MESH)
    swapped.wait_recv()
    layer_norm(tri_recv.reshape(ch, rows, lanes), tri_other.reshape(ch, rows, lanes))

    def close(k):
        v = (x_all[pl.ds(k, 2 * ch, stride=rows), :] * gain_all[1]).astype(BF16)
        y[pl.ds(k, ch, stride=rows), :] = jnp.dot(wo[...], v, preferred_element_type=F32) * gate[k]
    each(0, rows, close, 4)
    out[...] = y[...].reshape(ch, rows, lanes).astype(BF16)

    raw.wait_send()
    gsent.wait_send()
    swapped.wait_send()
    all_rows(send.at[0], left_recv, l_send, r_recv.at[0]).wait_send()
    for h in range(GROUPS):
        all_rows(right_recv.at[h], right_recv.at[h], r_send, r_recv.at[h]).wait_send()
        all_rows(tri_send.at[h], tri_send.at[h], t_send, r_recv.at[h]).wait_send()
    for d in range(1, nx):
        whole_col(d).wait_send()


def solution(mesh):
    n, nx = mesh.shape["row"], mesh.shape["col"]

    def per_device(pair_act, in_gain, left_proj, left_gate, right_proj, right_gate, out_gate, out_gain, out_proj):
        ch, rows, lanes = pair_act.shape
        hp = ch // n
        vm = pltpu.VMEM
        dma, reg = pltpu.SemaphoreType.DMA, pltpu.SemaphoreType.REGULAR
        return pl.pallas_call(
            functools.partial(kernel, n, nx),
            out_shape=pltpu.VMEM(pair_act.shape, BF16),
            in_specs=[pl.BlockSpec(memory_space=pl.ANY)] * 9,
            out_specs=pl.BlockSpec(memory_space=pltpu.VMEM),
            scratch_shapes=[
                vm((ch, rows, lanes), BF16),
                vm((ch, rows, lanes), BF16),
                vm((2, 1, ch), F32),
                vm((2, ch, lanes), F32),
                vm((2, ch, lanes), F32),
                vm((2, 2 * ch, lanes), F32),
                vm((2 * ch * rows, lanes), F32),
                vm((rows, 2 * ch, lanes), BF16),
                vm((5 * ch, 2 * ch), BF16),
                vm((ch, 2 * ch), BF16),
                vm((rows, ch, lanes), F32),
                vm((ch * rows, lanes), F32),
                vm((2, n, hp, rows, lanes), BF16),
                vm((n, hp, rows, lanes), BF16),
                vm((GROUPS, n, hp // GROUPS, rows, lanes), BF16),
                vm((nx, n, hp, rows, lanes), BF16),
                vm((GROUPS, n, hp // GROUPS, rows, lanes), BF16),
                vm((n, hp, rows, lanes), BF16),
                vm((n, hp, rows, lanes), BF16),
                reg((n,)),
                reg((nx,)),
                dma((9,)),
                dma((2,)),
                dma((2,)),
                dma,
                dma((n,)),
                dma,
                dma((GROUPS,)),
                dma,
                dma((nx,)),
                dma,
                dma((GROUPS, n)),
                dma,
                dma,
            ],
            compiler_params=pltpu.CompilerParams(collective_id=0, has_side_effects=True),
            name="triangle",
        )(pair_act, in_gain[None], left_proj.T, left_gate.T, right_proj.T, right_gate.T, out_gate.T, out_gain[None], out_proj.T)

    return jax.shard_map(
        per_device,
        mesh=mesh,
        in_specs=(
            P("ch", ("grp", "row"), "col"),
            P("ch"),
            P(None, "ch"),
            P(None, "ch"),
            P(None, "ch"),
            P(None, "ch"),
            P(None, "ch"),
            P("ch"),
            P(None, "ch"),
        ),
        out_specs=P("ch", ("grp", "row"), "col"),
        check_vma=False,
    )
```

```python
import functools

import jax
import jax.numpy as jnp
from jax import lax
from jax.experimental import pallas as pl
from jax.experimental.pallas import tpu as pltpu
from jax.sharding import PartitionSpec as P

MESH = pl.DeviceIdType.MESH
EPS = 1e-05
GROUPS = 1
F32, BF16 = jnp.float32, jnp.bfloat16


def kernel(n, nx, pa_in, ing, lp, lg, rp, rg, og, outg, op, out,
           pa, other, rows_in, gains, gains_other, gain_all, x_all, v_all, wt, wo, gate, y,
           send, left_recv, right_recv, left_all, tri_send, tri_recv, tri_other,
           ready, ready_x, in_sem, ch_send, ch_recv, l_send, l_recv, r_send, r_recv, x_send, x_recv, t_send, t_recv, o_send, o_recv):
    z, x, c = lax.axis_index("row"), lax.axis_index("col"), lax.axis_index("ch")
    ch, rows, lanes = pa.shape
    hp = ch // n
    per_group = hp // GROUPS
    turn = lax.rem(z + n - 1, n)
    bar = pltpu.get_barrier_semaphore()

    def each(lo, hi, f, unroll=None):
        def step(i, carry):
            f(i)
            return carry
        lax.fori_loop(lo, hi, step, 0, unroll=unroll)

    def row_at(i):
        return lax.rem(i + 1, n)

    def turn_of(r):
        return lax.rem(r + n - 1, n)

    def to_core(src, dst, i):
        return pltpu.make_async_remote_copy(src_ref=src, dst_ref=dst, send_sem=ch_send.at[i], recv_sem=ch_recv.at[i],
                                            device_id={"ch": 1 - c}, device_id_type=MESH)

    pl.semaphore_signal(bar, inc=1, device_id={"ch": 1 - c}, device_id_type=MESH)
    loads = [pltpu.make_async_copy(pa_in, pa, in_sem.at[0]),
             pltpu.make_async_copy(ing, rows_in.at[0], in_sem.at[1]),
             pltpu.make_async_copy(outg, rows_in.at[1], in_sem.at[2])]
    for i, w in enumerate((lp, lg, rp, rg, og)):
        loads.append(pltpu.make_async_copy(w, wt.at[pl.ds(i * ch, ch), :], in_sem.at[3 + i]))
    loads.append(pltpu.make_async_copy(op, wo, in_sem.at[8]))
    for load in loads:
        load.start()
    each(0, x, lambda r: pl.semaphore_signal(bar, inc=1, device_id={"col": r}, device_id_type=MESH))
    each(turn + 1, n, lambda i: pl.semaphore_signal(bar, inc=1, device_id={"row": row_at(i)}, device_id_type=MESH))
    pl.semaphore_wait(bar, turn + (nx - 1 - x) + 1)
    raw = to_core(pa, other, 0)
    loads[0].wait()
    raw.start()
    each(0, turn, lambda i: pl.semaphore_signal(ready.at[z], inc=1, device_id={"row": row_at(i)}, device_id_type=MESH))
    each(x + 1, nx, lambda r: pl.semaphore_signal(ready_x.at[x], inc=1, device_id={"col": r}, device_id_type=MESH))
    for load in loads[1:]:
        load.wait()
    for i in range(2):
        gains[i] = jnp.broadcast_to(rows_in[i], (lanes, ch)).T
    gsent = to_core(gains, gains_other, 1)
    gsent.start()
    mine = pl.multiple_of(c * ch, ch)
    theirs = pl.multiple_of((1 - c) * ch, ch)
    raw.wait_recv()
    step_c = 8

    def layer_norm(a, b):
        def add(i, t):
            s = pl.ds(i * step_c, step_c)
            return t + a[s].astype(F32).sum(0) + b[s].astype(F32).sum(0)
        mean = lax.fori_loop(0, ch // step_c, add, jnp.zeros((rows, lanes), F32)) / (2 * ch)

        def sq(i, t):
            s = pl.ds(i * step_c, step_c)
            return t + jnp.square(a[s].astype(F32) - mean).sum(0) + jnp.square(b[s].astype(F32) - mean).sum(0)
        var = lax.fori_loop(0, ch // step_c, sq, jnp.zeros((rows, lanes), F32)) / (2 * ch)
        scale = lax.rsqrt(var + EPS)

        def put(i, carry):
            s = pl.ds(i * step_c, step_c)
            for r, base in ((a, mine), (b, theirs)):
                v = (r[s].astype(F32) - mean) * scale
                x_all[pl.ds(pl.multiple_of((base + i * step_c) * rows, rows * step_c), rows * step_c), :] = v.reshape(rows * step_c, lanes)
            return carry
        lax.fori_loop(0, ch // step_c, put, 0)

    layer_norm(pa, other)
    gsent.wait_recv()
    for i in range(2):
        gain_all[i, pl.ds(mine, ch), :] = gains[i]
        gain_all[i, pl.ds(theirs, ch), :] = gains_other[i]
    def edges(v, i):
        r = jnp.dot(wt[pl.ds(2 * i * ch, 2 * ch), :], v, preferred_element_type=F32)
        return jax.nn.sigmoid(r[ch:]) * r[:ch]

    def lift_left(k):
        v = (x_all[pl.ds(k, 2 * ch, stride=rows), :] * gain_all[0]).astype(BF16)
        v_all[k] = v
        y[pl.ds(k, ch, stride=rows), :] = edges(v, 0)
    each(0, rows, lift_left, 8)

    def pack(side):
        def one(i):
            s = pl.ds(pl.multiple_of(i * hp * rows, hp * rows), hp * rows)
            send[side, i] = y[s, :].reshape(hp, rows, lanes).astype(BF16)
        each(0, n, one, 4)
    pack(0)

    def part(g):
        return pl.ds(g * per_group, per_group)

    def left_copy(r, slot):
        return pltpu.make_async_remote_copy(src_ref=send.at[0, r], dst_ref=left_recv.at[slot], send_sem=l_send, recv_sem=l_recv.at[slot],
                                            device_id={"row": r}, device_id_type=MESH)

    def right_copy(h, r, slot):
        return pltpu.make_async_remote_copy(src_ref=send.at[1, r, part(h)], dst_ref=right_recv.at[h, slot], send_sem=r_send, recv_sem=r_recv.at[h],
                                            device_id={"row": r}, device_id_type=MESH)

    def down_at(copy, i):
        d = n // 2 - i
        r1, r2 = lax.rem(z + d, n), lax.rem(z + n - d, n)

        @pl.when(turn_of(r1) < turn)
        def _():
            copy(r1, z).start()

        @pl.when((turn_of(r2) < turn) & (d < n // 2))
        def _():
            copy(r2, z).start()
    each(0, n // 2, functools.partial(down_at, left_copy))
    def lift_right(k):
        y[pl.ds(k, ch, stride=rows), :] = edges(v_all[k], 1)
    each(0, rows, lift_right, 4)
    pack(1)
    for h in range(GROUPS):
        right_recv[h, z] = send[1, z, h * per_group : (h + 1) * per_group]
    left_recv[z] = send[0, z]

    def down_right(i):
        for h in range(GROUPS):
            down_at(functools.partial(right_copy, h), i)

    def up_left(i):
        r = row_at(i)
        pl.semaphore_wait(ready.at[r], 1)
        left_copy(r, z).start()

    def up_right(i):
        for h in range(GROUPS):
            right_copy(h, row_at(i), z).start()

    def up(i):
        up_left(i)
        up_right(i)
    early = turn < n // 2
    ahead = jnp.where(early, n // 2, 0)
    each(0, ahead, down_right)
    half = jnp.maximum(turn + 1, n // 2)
    each(turn + 1, half, up)

    def mixed(i):
        up_left(i)
        t = ahead + i - turn - 1

        @pl.when(t < n // 2)
        def _():
            down_right(t)
    each(half, n, mixed)
    each(jnp.minimum(ahead + n - half, n // 2), n // 2, down_right)
    each(half, n, up_right)
    def lift_gate(k):
        gate[k] = jax.nn.sigmoid(jnp.dot(wt[pl.ds(4 * ch, ch), :], v_all[k], preferred_element_type=F32))
    each(0, rows, lift_gate, 4)
    each(0, x, lambda r: pl.semaphore_wait(ready_x.at[r], 1))

    def to_col(s, r):
        return pltpu.make_async_remote_copy(src_ref=left_recv.at[s], dst_ref=left_all.at[x, s], send_sem=x_send, recv_sem=x_recv.at[x],
                                            device_id={"col": r}, device_id_type=MESH)

    def spread(s):
        for d in range(1, nx):
            to_col(s, lax.rem(x + d, nx)).start()
        left_all[x, s] = left_recv[s]

    def arrived(s):
        left_copy(s, s).wait_recv()
        spread(s)
    spread(z)

    last = turn >= n - n // 4

    def in_order(i):
        @pl.when(i != turn)
        def _():
            arrived(row_at(i))
    each(0, jnp.where(last, 0, n), in_order)

    def farthest(i):
        d = n // 2 - i
        arrived(lax.rem(z + d, n))

        @pl.when(d < n // 2)
        def _():
            arrived(lax.rem(z + n - d, n))
    each(jnp.where(last, 0, n // 2), n // 2, farthest)

    def all_rows(src, dst, ss, rs):
        most = pl.ds(0, n - 1)
        return pltpu.make_async_remote_copy(src_ref=src.at[most], dst_ref=dst.at[most], send_sem=ss, recv_sem=rs,
                                            device_id={"row": lax.rem(z + 1, n)}, device_id_type=MESH)

    def whole_col(d):
        r = lax.rem(x + d, nx)
        return pltpu.make_async_remote_copy(src_ref=left_all.at[r], dst_ref=left_all.at[r], send_sem=x_send, recv_sem=x_recv.at[r],
                                            device_id={"col": r}, device_id_type=MESH)
    for d in range(1, nx):
        whole_col(d).wait_recv()
    def tri_copy(h, r, slot):
        return pltpu.make_async_remote_copy(src_ref=tri_send.at[h, r], dst_ref=tri_recv.at[slot, part(h)], send_sem=t_send, recv_sem=t_recv.at[h, slot],
                                            device_id={"row": r}, device_id_type=MESH)

    def swap(h, s):
        return pltpu.make_async_remote_copy(src_ref=tri_recv.at[s, part(h)], dst_ref=tri_other.at[s, part(h)], send_sem=o_send, recv_sem=o_recv,
                                            device_id={"ch": 1 - c}, device_id_type=MESH)

    per = lanes // rows
    for h in range(GROUPS):
        all_rows(right_recv.at[h], right_recv.at[h], r_send, r_recv.at[h]).wait_recv()
        rights = [right_recv[h, :, m].reshape(n * rows, lanes) for m in range(per_group)]

        def tri_block(q):
            for m in range(per_group):
                left = left_all[q, :, h * per_group + m].reshape(n * rows, lanes)
                t = lax.dot_general(left, rights[m], (((0,), (0,)), ((), ())), preferred_element_type=F32)
                tri_send[h, pl.ds(pl.multiple_of(q * per, per), per), m] = t.reshape(per, rows, lanes).astype(BF16)

        def tri_to(r):
            @pl.when(r != z)
            def _():
                tri_copy(h, r, z).start()

        def far_block(q):
            tri_block(q)
            each(0, per, lambda k: tri_to(q * per + k))
        for off in sorted(range(nx), key=lambda o: -min(o, nx - o)):
            far_block(lax.rem(z // per + off, nx))
        tri_recv[z, h * per_group : (h + 1) * per_group] = tri_send[h, z]

    for h in range(GROUPS):
        swap(h, z).start()

        def tri_in(i):
            d = n // 2 - i
            r1, r2 = lax.rem(z + d, n), lax.rem(z + n - d, n)
            tri_copy(h, r1, r1).wait_recv()
            swap(h, r1).start()

            @pl.when(d < n // 2)
            def _():
                tri_copy(h, r2, r2).wait_recv()
                swap(h, r2).start()
        each(0, n // 2, tri_in)
    swapped = pltpu.make_async_remote_copy(src_ref=tri_recv, dst_ref=tri_other, send_sem=o_send, recv_sem=o_recv,
                                           device_id={"ch": 1 - c}, device_id_type=MESH)
    swapped.wait_recv()
    layer_norm(tri_recv.reshape(ch, rows, lanes), tri_other.reshape(ch, rows, lanes))

    def close(k):
        v = (x_all[pl.ds(k, 2 * ch, stride=rows), :] * gain_all[1]).astype(BF16)
        y[pl.ds(k, ch, stride=rows), :] = jnp.dot(wo[...], v, preferred_element_type=F32) * gate[k]
    each(0, rows, close, 4)
    out[...] = y[...].reshape(ch, rows, lanes).astype(BF16)

    raw.wait_send()
    gsent.wait_send()
    swapped.wait_send()
    all_rows(send.at[0], left_recv, l_send, r_recv.at[0]).wait_send()
    for h in range(GROUPS):
        all_rows(right_recv.at[h], right_recv.at[h], r_send, r_recv.at[h]).wait_send()
        all_rows(tri_send.at[h], tri_send.at[h], t_send, r_recv.at[h]).wait_send()
    for d in range(1, nx):
        whole_col(d).wait_send()


def solution(mesh):
    n, nx = mesh.shape["row"], mesh.shape["col"]

    def per_device(pair_act, in_gain, left_proj, left_gate, right_proj, right_gate, out_gate, out_gain, out_proj):
        ch, rows, lanes = pair_act.shape
        hp = ch // n
        vm = pltpu.VMEM
        dma, reg = pltpu.SemaphoreType.DMA, pltpu.SemaphoreType.REGULAR
        return pl.pallas_call(
            functools.partial(kernel, n, nx),
            out_shape=pltpu.VMEM(pair_act.shape, BF16),
            in_specs=[pl.BlockSpec(memory_space=pl.ANY)] * 9,
            out_specs=pl.BlockSpec(memory_space=pltpu.VMEM),
            scratch_shapes=[
                vm((ch, rows, lanes), BF16),
                vm((ch, rows, lanes), BF16),
                vm((2, 1, ch), F32),
                vm((2, ch, lanes), F32),
                vm((2, ch, lanes), F32),
                vm((2, 2 * ch, lanes), F32),
                vm((2 * ch * rows, lanes), F32),
                vm((rows, 2 * ch, lanes), BF16),
                vm((5 * ch, 2 * ch), BF16),
                vm((ch, 2 * ch), BF16),
                vm((rows, ch, lanes), F32),
                vm((ch * rows, lanes), F32),
                vm((2, n, hp, rows, lanes), BF16),
                vm((n, hp, rows, lanes), BF16),
                vm((GROUPS, n, hp // GROUPS, rows, lanes), BF16),
                vm((nx, n, hp, rows, lanes), BF16),
                vm((GROUPS, n, hp // GROUPS, rows, lanes), BF16),
                vm((n, hp, rows, lanes), BF16),
                vm((n, hp, rows, lanes), BF16),
                reg((n,)),
                reg((nx,)),
                dma((9,)),
                dma((2,)),
                dma((2,)),
                dma,
                dma((n,)),
                dma,
                dma((GROUPS,)),
                dma,
                dma((nx,)),
                dma,
                dma((GROUPS, n)),
                dma,
                dma,
            ],
            compiler_params=pltpu.CompilerParams(collective_id=0, has_side_effects=True),
            name="triangle",
        )(pair_act, in_gain[None], left_proj.T, left_gate.T, right_proj.T, right_gate.T, out_gate.T, out_gain[None], out_proj.T)

    return jax.shard_map(
        per_device,
        mesh=mesh,
        in_specs=(
            P("ch", ("grp", "row"), "col"),
            P("ch"),
            P(None, "ch"),
            P(None, "ch"),
            P(None, "ch"),
            P(None, "ch"),
            P(None, "ch"),
            P("ch"),
            P(None, "ch"),
        ),
        out_specs=P("ch", ("grp", "row"), "col"),
        check_vma=False,
    )
```
